32 devices in a mesh: blk: 16 (over z, y, core), team: 2 (over x).
Axes of the slice: x: 2, y: 2, z: 4, core: 2. Of those that a mesh axis runs over, the one named last changes fastest.
Arguments:
- positions: float32 [16384, 3], P('blk'), may hold values from 0 to 1
- velocity: float32 [16384, 3], P('blk'), may hold values from -6 to 6
- masses: float32 [16384], P('blk'), may hold values from 6.1035157e-06 to 0.00061035156
Outputs:
- accel: float32 [16384, 3], P('blk')
- velocity_next: float32 [16384, 3], P('blk')
- positions_next: float32 [16384, 3], P('blk')
The draws below stay inside these ranges and needn't reach their ends.
All inputs are finite; a program needn't handle non-finite values.
Results may differ from the reference program's by a relative error of at most 0.0003.
Values sent between devices are 32-bit elements.
A program may use at most 64 MiB of HBM per device.

```python
import math
import jax
import jax.numpy as jnp
from jax import lax

BODY_DEV = 1024
BODIES = 16384
N_BLK = 16


def level_of(stream_key, dims, pieces, smallest, top_value):
    def one(axis_at, shards_of):
        heights = jax.random.uniform(jax.random.fold_in(jax.random.fold_in(stream_key, 6), axis_at), (shards_of,), jnp.float32, smallest / len(pieces), top_value / len(pieces))
        return jnp.repeat(jnp.exp(heights), dims[axis_at] // shards_of).reshape((-1,) + (1,) * (len(dims) - axis_at - 1))

    factor_of = one(*pieces[0])
    for cut in pieces[1:]:
        factor_of = factor_of * one(*cut)
    return factor_of


def bell_draw(stream_key, shape, width, bound, split=(), held_as=jnp.bfloat16):
    array = jax.random.normal(stream_key, shape, jnp.float32) * width
    if len(split) > 0:
        array = level_of(stream_key, shape, split, -0.22, 0.18) * array
    return jnp.clip(array, min=-bound, max=bound).astype(held_as)


def setup_inputs(seed: int = 0) -> dict:
    key_list = jax.random.split(jax.random.key(seed), 4)
    return {
        "positions": jnp.clip(1.0 * jax.random.uniform(key_list[0], (BODIES, 3), jnp.float32) ** level_of(key_list[0], (BODIES, 3), ((0, 16),), -0.2, 0.2), 0.0, 1.0),
        "velocity": bell_draw(key_list[1], (BODIES, 3), 1.0, 6.0, ((0, 16),), jnp.float32),
        "masses": jnp.clip(jnp.exp(math.log(0.00061035156) - 4.6051702 * jax.random.uniform(key_list[2], (BODIES,), jnp.float32) ** level_of(key_list[2], (BODIES,), ((0, 16),), -0.2, 0.2)), 6.10351571594947e-06, 0.00061035156),
    }


SOFTEN_SQ = 0.0004
TIME_STEP = 0.01

def attract(targets, src_pos, src_mass):
    deltas = [src_pos[None, :, column] - targets[:, column:column + 1] for column in range(3)]
    dist_sq = deltas[0] * deltas[0] + deltas[1] * deltas[1] + deltas[2] * deltas[2] + SOFTEN_SQ
    inverse = lax.rsqrt(dist_sq)
    weight = src_mass[None, :] * inverse * inverse * inverse
    return jnp.stack([lax.optimization_barrier(jnp.sum(weight * delta, axis=1)) for delta in deltas], axis=1)

def reference(positions, velocity, masses):
    span_rows = BODY_DEV * math.gcd(N_BLK, 8)
    src_pos = positions.reshape(BODIES // span_rows, span_rows, 3)
    src_mass = masses.reshape(BODIES // span_rows, span_rows)
    target_blocks = positions.reshape(N_BLK, BODY_DEV, 3)

    def one_block(targets):

        def advance(summed, source):
            return (summed + attract(targets, source[0], source[1]), None)
        summed, unused = lax.scan(advance, jnp.zeros((BODY_DEV, 3), jnp.float32), (src_pos, src_mass))
        return summed
    accel = lax.map(one_block, target_blocks).reshape(BODIES, 3)
    velocity_next = velocity + TIME_STEP * accel
    positions_next = positions + TIME_STEP * velocity_next
    return (accel, velocity_next, positions_next)
```

```python
import functools

import jax
import jax.numpy as jnp
from jax import lax
from jax.experimental import pallas as pl
from jax.experimental.pallas import tpu as pltpu
from jax.sharding import PartitionSpec as P

SOFTEN_SQ = 0.0004
TIME_STEP = 0.01
MESH = pl.DeviceIdType.MESH
CHUNK = 256


def split3(values):
    high = values.astype(jnp.bfloat16).astype(jnp.float32)
    rest = values - high
    middle = rest.astype(jnp.bfloat16).astype(jnp.float32)
    return high, middle, rest - middle


def kernel(
    blocks, team, pos_ref, vel_ref, mass_ref, acc_out, vel_out, pos_out,
    held, feats, total, mine, theirs, send_sem, recv_sem, part_send, part_recv,
):
    me = lax.axis_index("blk")
    member = lax.axis_index("team")
    rows = pos_ref.shape[1]
    share = rows // team

    barrier = pltpu.get_barrier_semaphore()

    def greet(step, carry):
        pl.semaphore_signal(
            barrier, inc=1, device_id=(lax.rem(me + step, blocks), member), device_id_type=MESH
        )
        return carry

    lax.fori_loop(1, blocks, greet, 0)
    for step in range(1, team):
        pl.semaphore_signal(
            barrier, inc=1, device_id=(me, lax.rem(member + step, team)), device_id_type=MESH
        )

    first = pl.multiple_of(member * share, share)
    held[0, 0:3, :] = pos_ref[:, pl.ds(first, share)]
    held[0, 3:4, :] = mass_ref[:, pl.ds(first, share)]

    pos = pos_ref[...]
    centre = jnp.sum(pos, axis=1, keepdims=True) * (1.0 / rows)
    near = pos - centre
    norm = jnp.sum(near * near, axis=0, keepdims=True) + SOFTEN_SQ
    target = jnp.concatenate(
        [-2.0 * near, jnp.ones((1, rows), jnp.float32), norm, jnp.zeros((3, rows), jnp.float32)], axis=0
    )
    high, middle, low = split3(target)
    feats[...] = jnp.concatenate([high, middle, high, middle, low, high], axis=0).astype(jnp.bfloat16)
    total[...] = jnp.zeros_like(total)

    pl.semaphore_wait(barrier, blocks - 1 + team - 1)

    def passing(step):
        return pltpu.make_async_remote_copy(
            src_ref=held.at[0],
            dst_ref=held.at[step],
            send_sem=send_sem.at[step],
            recv_sem=recv_sem.at[step],
            device_id=(lax.rem(me + step, blocks), member),
            device_id_type=MESH,
        )

    def send(step, carry):
        passing(step).start()
        return carry

    lax.fori_loop(1, blocks, send, 0)

    def attract(step):
        block = held[step]
        away = block[0:3] - centre
        weight = block[3:4]
        square = jnp.sum(away * away, axis=0, keepdims=True)
        source = jnp.concatenate(
            [away, square, jnp.ones((1, share), jnp.float32), jnp.zeros((3, share), jnp.float32)], axis=0
        )
        high, middle, low = split3(source)
        left = jnp.concatenate([high, high, middle, middle, high, low], axis=0)
        left = jnp.transpose(left).astype(jnp.bfloat16)
        moment = jnp.concatenate(
            [away * weight, weight, jnp.zeros((4, share), jnp.float32)], axis=0
        )
        moments = jnp.concatenate(split3(moment), axis=0).astype(jnp.bfloat16)
        for start in range(0, rows, CHUNK):
            columns = slice(start, start + CHUNK)
            dist_sq = jnp.dot(left, feats[:, columns], preferred_element_type=jnp.float32)
            inverse = lax.rsqrt(dist_sq)
            cube = inverse * inverse * inverse
            upper = cube.astype(jnp.bfloat16)
            lower = (cube - upper.astype(jnp.float32)).astype(jnp.bfloat16)
            total[:, columns] += jnp.dot(
                moments, upper, preferred_element_type=jnp.float32
            ) + jnp.dot(moments, lower, preferred_element_type=jnp.float32)

    attract(0)

    def arrive(step, carry):
        passing(step).wait_recv()
        attract(step)
        return carry

    lax.fori_loop(1, blocks, arrive, 0)

    summed = total[0:8, :] + total[8:16, :] + total[16:24, :]
    mine[...] = summed[0:3] - near * summed[3:4]
    copies = [
        pltpu.make_async_remote_copy(
            src_ref=mine,
            dst_ref=theirs.at[step],
            send_sem=part_send.at[step],
            recv_sem=part_recv.at[step],
            device_id=(me, lax.rem(member + step, team)),
            device_id_type=MESH,
        )
        for step in range(1, team)
    ]
    for copy in copies:
        copy.start()

    def sent(step, carry):
        passing(step).wait_send()
        return carry

    lax.fori_loop(1, blocks, sent, 0)
    accel = mine[...]
    for step, copy in enumerate(copies):
        copy.wait()
        accel = accel + theirs[step + 1]
    velocity_next = vel_ref[...] + TIME_STEP * accel
    acc_out[...] = accel
    vel_out[...] = velocity_next
    pos_out[...] = pos + TIME_STEP * velocity_next


def per_device(positions, velocity, masses):
    blocks, team = lax.axis_size("blk"), lax.axis_size("team")
    rows = positions.shape[0]
    share = rows // team
    wide = jax.ShapeDtypeStruct((3, rows), jnp.float32)
    outs = pl.pallas_call(
        functools.partial(kernel, blocks, team),
        out_shape=(wide, wide, wide),
        in_specs=[pl.BlockSpec(memory_space=pltpu.VMEM)] * 3,
        out_specs=(pl.BlockSpec(memory_space=pltpu.VMEM),) * 3,
        scratch_shapes=[
            pltpu.VMEM((blocks, 4, share), jnp.float32),
            pltpu.VMEM((48, rows), jnp.bfloat16),
            pltpu.VMEM((24, rows), jnp.float32),
            pltpu.VMEM((3, rows), jnp.float32),
            pltpu.VMEM((team, 3, rows), jnp.float32),
            pltpu.SemaphoreType.DMA((blocks,)),
            pltpu.SemaphoreType.DMA((blocks,)),
            pltpu.SemaphoreType.DMA((team,)),
            pltpu.SemaphoreType.DMA((team,)),
        ],
        compiler_params=pltpu.CompilerParams(collective_id=0, has_side_effects=True),
    )(positions.T, velocity.T, masses.reshape(1, rows))
    return tuple(out.T for out in outs)


def solution(mesh):
    in_specs = (P("blk", None), P("blk", None), P("blk"))
    out_specs = (P("blk", None), P("blk", None), P("blk", None))
    return jax.shard_map(
        per_device, mesh=mesh, in_specs=in_specs, out_specs=out_specs, check_vma=False
    )
```
